32 devices in a mesh: grp: 2 (over y), pen: 8 (over z, x), ch: 2 (over core).
Axes of the slice: x: 2, y: 2, z: 4, core: 2. Of those that a mesh axis runs over, the one named last changes fastest.
Arguments:
- features: bfloat16 [256, 32, 128, 256], P(('grp', 'pen'), 'ch'), parts along dimension 0, may hold values from -6 to 6
- spectral_weights: bfloat16 [1, 2, 16, 32, 32, 1024], P(None, None, None, None, 'ch', 'pen'), may hold values from -0.75 to 0.75
- bypass_weights: float32 [1, 32, 32], P(None, None, 'ch'), may hold values from -0.75 to 0.75
- bypass_bias: float32 [1, 32], P(None, 'ch'), may hold values from -1 to 1
Outputs:
- features_out: float32 [256, 32, 128, 256], P(('grp', 'pen'), 'ch'), parts along dimension 0
The draws below stay inside these ranges and needn't reach their ends.
There are 2 independent parts, one for each index of `grp`. The reference program is written for one: setup_inputs(seed, part) draws one part's arguments, and reference() takes and returns one part's arrays. A program takes and returns all parts, laid end to end along the dimension named above; an argument that names none is the same for every part. Nothing has to cross between parts.
All inputs are finite; a program needn't handle non-finite values.
Results may differ from the reference program's by a relative error of at most 0.0003.
Values may be sent and summed in bfloat16 or wider, within the bound.
A program may use at most 192 MiB of HBM per device.

```python
import math
import jax
import jax.numpy as jnp
from jax import lax

C = 32
NX = 128
NY = 128
NZ = 256
MX = 16
MY = 32
MZ = 32
LAYERS = 1


def steps_of(key, dims, shards, low, largest):
    factor_of, own = 1.0, jax.random.fold_in(key, 6)
    for axis_at, blocks in shards:
        draws = jnp.exp(jax.random.uniform(jax.random.fold_in(own, axis_at), (blocks,), jnp.float32, low / len(shards), largest / len(shards)))
        factor_of = factor_of * jnp.repeat(draws, dims[axis_at] // blocks).reshape([-1 if axis == axis_at else 1 for axis in range(len(dims))])
    return factor_of


def noise(key, shape, deviation, reach, cuts=(), kind=jnp.bfloat16):
    values = deviation * jax.random.normal(key, shape, jnp.float32)
    if cuts:
        values = values * steps_of(key, shape, cuts, -0.22, 0.18)
    return jnp.clip(values, -reach, reach).astype(kind)


def setup_inputs(seed: int = 0, part: int = 0) -> dict:
    streams_of = jax.random.split(jax.random.key(seed), 5)
    own_keys = jax.random.split(jax.random.fold_in(streams_of[4], part), 5)
    return {
        "features": noise(own_keys[0], (NX, C, NY, NZ), 1.0, 6.0, ((0, 8), (1, 2))),
        "spectral_weights": noise(streams_of[1], (LAYERS, 2, MX, C, C, MY * MZ), (2 * C) ** -0.5, 0.75, ((4, 2), (5, 8))),
        "bypass_weights": noise(streams_of[2], (LAYERS, C, C), (2 * C) ** -0.5, 0.75, ((2, 2),), jnp.float32),
        "bypass_bias": jnp.clip(jax.random.uniform(streams_of[3], (LAYERS, C), jnp.float32, -1.0, 1.0) * steps_of(streams_of[3], (LAYERS, C), ((1, 2),), -0.4, 0.0), -1.0, 1.0),
    }


HIGHEST = lax.Precision.HIGHEST


def kept_freqs(length, kept_count):
    offsets = jnp.arange(kept_count, dtype=jnp.int32)
    return jnp.where(offsets < kept_count // 2, offsets, length - kept_count + offsets)


def tables(length, kept_count):
    phases = (kept_freqs(length, kept_count)[:, None] * jnp.arange(length, dtype=jnp.int32)[None, :]) % length
    angles = phases.astype(jnp.float32) * (2.0 * math.pi / length)
    return jnp.cos(angles), jnp.sin(angles)


def reference(features, spectral_weights, bypass_weights, bypass_bias):
    cos_x, sin_x = tables(NX, MX)
    cos_y, sin_y = tables(NY, MY)
    cos_z, sin_z = tables(NZ, MZ)

    def forward_slab(x_slab):
        real_z = jnp.einsum('cyz,kz->cyk', x_slab, cos_z, precision=HIGHEST) * NZ ** -0.5
        imag_z = -jnp.einsum('cyz,kz->cyk', x_slab, sin_z, precision=HIGHEST) * NZ ** -0.5
        real_y = (jnp.einsum('ay,cyk->cak', cos_y, real_z, precision=HIGHEST)
                  + jnp.einsum('ay,cyk->cak', sin_y, imag_z, precision=HIGHEST)) * NY ** -0.5
        imag_y = (jnp.einsum('ay,cyk->cak', cos_y, imag_z, precision=HIGHEST)
                  - jnp.einsum('ay,cyk->cak', sin_y, real_z, precision=HIGHEST)) * NY ** -0.5
        return real_y, imag_y

    current = features.astype(jnp.float32)
    for layer_idx in range(LAYERS):
        real_y, imag_y = lax.map(forward_slab, current)
        real_x = (jnp.einsum('jx,xcak->jcak', cos_x, real_y, precision=HIGHEST)
                  + jnp.einsum('jx,xcak->jcak', sin_x, imag_y, precision=HIGHEST)) * NX ** -0.5
        imag_x = (jnp.einsum('jx,xcak->jcak', cos_x, imag_y, precision=HIGHEST)
                  - jnp.einsum('jx,xcak->jcak', sin_x, real_y, precision=HIGHEST)) * NX ** -0.5
        weights = spectral_weights[layer_idx].astype(jnp.float32).reshape(2, MX, C, C, MY, MZ)
        real_g = (jnp.einsum('jiak,jioak->joak', real_x, weights[0], precision=HIGHEST)
                  - jnp.einsum('jiak,jioak->joak', imag_x, weights[1], precision=HIGHEST))
        imag_g = (jnp.einsum('jiak,jioak->joak', imag_x, weights[0], precision=HIGHEST)
                  + jnp.einsum('jiak,jioak->joak', real_x, weights[1], precision=HIGHEST))
        real_h = (jnp.einsum('jx,joak->xoak', cos_x, real_g, precision=HIGHEST)
                  - jnp.einsum('jx,joak->xoak', sin_x, imag_g, precision=HIGHEST)) * MX ** -0.5
        imag_h = (jnp.einsum('jx,joak->xoak', cos_x, imag_g, precision=HIGHEST)
                  + jnp.einsum('jx,joak->xoak', sin_x, real_g, precision=HIGHEST)) * MX ** -0.5
        mixing = bypass_weights[layer_idx].astype(jnp.float32)
        offsets = bypass_bias[layer_idx].astype(jnp.float32)

        def inverse_slab(pieces, mixing=mixing, offsets=offsets):
            x_slab, real_b, imag_b = pieces
            real_a = (jnp.einsum('ay,oak->oyk', cos_y, real_b, precision=HIGHEST)
                      - jnp.einsum('ay,oak->oyk', sin_y, imag_b, precision=HIGHEST)) * MY ** -0.5
            imag_a = (jnp.einsum('ay,oak->oyk', cos_y, imag_b, precision=HIGHEST)
                      + jnp.einsum('ay,oak->oyk', sin_y, real_b, precision=HIGHEST)) * MY ** -0.5
            spectral = (jnp.einsum('oyk,kz->oyz', real_a, cos_z, precision=HIGHEST)
                        - jnp.einsum('oyk,kz->oyz', imag_a, sin_z, precision=HIGHEST)) * MZ ** -0.5
            bypass = jnp.einsum('io,iyz->oyz', mixing, x_slab, precision=HIGHEST)
            return x_slab + jax.nn.gelu(bypass + offsets[:, None, None] + spectral, approximate=True)

        current = lax.map(inverse_slab, (current, real_h, imag_h))
    return current
```

```python
import functools
import math

import jax
import jax.numpy as jnp
import ml_dtypes
import numpy as np
from jax import lax
from jax.experimental import pallas as pl
from jax.experimental.pallas import tpu as pltpu
from jax.sharding import PartitionSpec as P

HIGHEST = lax.Precision.HIGHEST
LANES = 128
MZ = 32
F32 = jnp.float32
BF16 = jnp.bfloat16


def tables(length, kept):
    offsets = np.arange(kept)
    freqs = np.where(offsets < kept // 2, offsets, length - kept + offsets)
    phases = (freqs[:, None] * np.arange(length)[None, :]) % length
    angles = phases.astype(np.float64) * (2.0 * math.pi / length)
    return np.cos(angles), np.sin(angles)


def split_np(table):
    table = table.astype(np.float32)
    high = table.astype(ml_dtypes.bfloat16)
    low = (table - high.astype(np.float32)).astype(ml_dtypes.bfloat16)
    return high, low


def split(value):
    high = value.astype(BF16)
    return high, (value - high.astype(F32)).astype(BF16)


def dot(left, right):
    return jnp.dot(left, right, preferred_element_type=F32)


def forward_kernel(x_ref, ty_ref, bh_ref, bl_ref, out_ref, y_ref, *, my, nsub):
    block, ch, _, nz = x_ref.shape
    parts = nz // LANES
    groups = my // nsub
    half = my * ch
    for b in range(block):
        for c in range(ch):
            both = dot(ty_ref[...], x_ref[b, c])
            rows = both[: 2 * my] + both[2 * my :]
            for part in range(parts):
                y_ref[b, part, pl.ds(c, 2 * my, stride=ch), :] = rows[
                    :, part * LANES : (part + 1) * LANES
                ]
    highs, lows = [], []
    for b in range(block):
        pieces = []
        for cs in range(2):
            loaded = [
                y_ref[b, part, cs * half : (cs + 1) * half, :].reshape(groups, nsub, ch, LANES)
                for part in range(parts)
            ]
            for sub in range(nsub):
                for part in range(parts):
                    pieces.append(loaded[part][:, sub].reshape(groups * ch, LANES))
        high, low = split(jnp.concatenate(pieces, axis=1))
        highs.append(high)
        lows.append(low)
    high = jnp.concatenate(highs, axis=0)
    low = jnp.concatenate(lows, axis=0)
    result = dot(high, bh_ref[...]) + dot(low, bh_ref[...]) + dot(high, bl_ref[...])
    result = result.reshape(block, groups, ch, 2 * LANES)
    for b in range(block):
        out_ref[:, b] = result[b]


def inverse_kernel(
    cx_ref, who_ref, g_ref, x_ref, mix_ref, bias_ref, zh_ref, zl_ref, ty_ref, out_ref, v_ref, w_ref
    , *, my, nsub, ysub
):
    step = pl.program_id(0)
    groups, mx, ch, _ = g_ref.shape
    _, all_ch, ny, nz = x_ref.shape
    parts = nz // LANES

    @pl.loop(0, groups)
    def _(group):
        real = jnp.zeros((ch, LANES), F32)
        imag = jnp.zeros((ch, LANES), F32)
        for j in range(mx):
            cos, sin = cx_ref[step, j], cx_ref[step, mx + j]
            g_re = g_ref[group, j, :, :LANES]
            g_im = g_ref[group, j, :, LANES:]
            real = real + (g_re * cos - g_im * sin)
            imag = imag + (g_im * cos + g_re * sin)
        v_ref[group, :, :LANES] = real
        v_ref[group, :, LANES:] = imag

    high, low = split(v_ref[...].reshape(groups * ch, 2 * LANES))
    for piece in range(nsub * 2):
        cols = slice(piece * nz, (piece + 1) * nz)
        waves = dot(high, zh_ref[:, cols]) + dot(low, zh_ref[:, cols]) + dot(high, zl_ref[:, cols])
        for part in range(parts):
            w_ref[piece, part] = waves[:, part * LANES : (part + 1) * LANES]
    for o in range(ch):
        rows = jnp.concatenate(
            [
                jnp.concatenate(
                    [w_ref[piece, part, pl.ds(o, groups, stride=ch), :] for part in range(parts)],
                    axis=1,
                )
                for piece in range(nsub * 2)
            ],
            axis=0,
        )
        high, low = split(rows)
        spectral = dot(ty_ref[...], jnp.concatenate([high, high, low], axis=0))
        out_ref[0, o] = spectral + bias_ref[0, o]
    first = who_ref[0]
    for at in range(0, ny, ysub):
        window = slice(at, at + ysub)
        cells = x_ref[0, :, window, :].reshape(all_ch * ysub, nz)
        bypass = dot(mix_ref[...], jnp.concatenate([cells, cells], axis=0))
        inner = bypass.reshape(ch, ysub, nz) + out_ref[0, :, window, :]
        own = x_ref[0, pl.ds(first, ch), window, :].astype(F32)
        cubic = inner * (1.0 + 0.044715 * (inner * inner))
        out_ref[0, :, window, :] = own + 0.5 * inner * (
            1.0 + jnp.tanh(math.sqrt(2.0 / math.pi) * cubic)
        )


def whole_vmem():
    return pl.BlockSpec(memory_space=pltpu.VMEM)


def forward_modes(features, my, mz):
    slabs, ch, ny, nz = features.shape
    nsub = LANES // mz
    groups = my // nsub
    cos_y, sin_y = tables(ny, my)
    cos_z, sin_z = tables(nz, mz)
    y_table = np.concatenate(split_np(np.concatenate([cos_y, sin_y]) * ny**-0.5), axis=0)
    pair = np.stack([np.stack([cos_z, -sin_z]), np.stack([-sin_z, -cos_z])]) * nz**-0.5
    z_table = np.einsum("crkz,st->cszrtk", pair, np.eye(nsub)).reshape(2 * nsub * nz, 2 * LANES)
    z_high, z_low = split_np(z_table)
    block = 2 if slabs % 2 == 0 else 1
    return pl.pallas_call(
        functools.partial(forward_kernel, my=my, nsub=nsub),
        grid=(slabs // block,),
        in_specs=[
            pl.BlockSpec((block, ch, ny, nz), lambda i: (i, 0, 0, 0)),
            whole_vmem(),
            whole_vmem(),
            whole_vmem(),
        ],
        out_specs=pl.BlockSpec((groups, block, ch, 2 * LANES), lambda i: (0, i, 0, 0)),
        out_shape=jax.ShapeDtypeStruct((groups, slabs, ch, 2 * LANES), F32),
        scratch_shapes=[pltpu.VMEM((block, nz // LANES, 2 * my * ch, LANES), F32)],
        compiler_params=pltpu.CompilerParams(vmem_limit_bytes=48 * 2**20),
        name="forward_modes",
    )(features, jnp.asarray(y_table), jnp.asarray(z_high), jnp.asarray(z_low))


def inverse_field(coefs, first, modes, gathered, mixing, bias, my, mz):
    slabs, all_ch, ny, nz = gathered.shape
    groups, mx, ch, _ = modes.shape
    nsub = LANES // mz
    ysub = 16
    cos_y, sin_y = tables(ny, my)
    cos_z, sin_z = tables(nz, mz)
    pair = np.stack([np.stack([cos_z, sin_z]), np.stack([-sin_z, cos_z])]) * mz**-0.5
    z_table = np.einsum("rckz,ts->rtkscz", pair, np.eye(nsub)).reshape(2 * LANES, 2 * nsub * nz)
    z_high, z_low = split_np(z_table)
    y_pair = np.stack([cos_y, -sin_y]).reshape(2, groups, nsub, ny) * my**-0.5
    y_high, y_low = split_np(y_pair.transpose(3, 2, 0, 1).reshape(ny, 2 * my))
    y_table = np.concatenate([y_high, y_low, y_high], axis=1)
    high = lax.reduce_precision(mixing, 8, 7)
    both = jnp.stack([high, mixing - high]).astype(BF16)
    eye = jnp.eye(ysub, dtype=BF16)
    mix = (
        both.transpose(2, 0, 1)[:, None, :, :, None] * eye[None, :, None, None, :]
    ).reshape(ch * ysub, 2 * all_ch * ysub)
    return pl.pallas_call(
        functools.partial(inverse_kernel, my=my, nsub=nsub, ysub=ysub),
        grid=(slabs,),
        in_specs=[
            pl.BlockSpec(memory_space=pltpu.SMEM),
            pl.BlockSpec(memory_space=pltpu.SMEM),
            whole_vmem(),
            pl.BlockSpec((1, all_ch, ny, nz), lambda i: (i, 0, 0, 0)),
            whole_vmem(),
            pl.BlockSpec(memory_space=pltpu.SMEM),
            whole_vmem(),
            whole_vmem(),
            whole_vmem(),
        ],
        out_specs=pl.BlockSpec((1, ch, ny, nz), lambda i: (i, 0, 0, 0)),
        out_shape=jax.ShapeDtypeStruct((slabs, ch, ny, nz), F32),
        scratch_shapes=[
            pltpu.VMEM((groups, ch, 2 * LANES), F32),
            pltpu.VMEM((2 * nsub, nz // LANES, groups * ch, LANES), F32),
        ],
        compiler_params=pltpu.CompilerParams(vmem_limit_bytes=60 * 2**20),
        name="inverse_field",
    )(
        coefs,
        first,
        modes,
        gathered,
        mix,
        bias,
        jnp.asarray(z_high),
        jnp.asarray(z_low),
        jnp.asarray(y_table),
    )


def local(features, spectral_weights, bypass_weights, bypass_bias, *, pens, kept):
    slabs, ch, ny, nz = features.shape
    _, _, mx, all_ch, _, owned = spectral_weights.shape
    nx = slabs * pens
    mz = MZ
    my = kept // mz
    groups = kept // LANES
    gathered = lax.all_gather(features, "ch", axis=1, tiled=True)
    modes = forward_modes(features, my, mz)
    if owned != LANES:
        modes = modes.reshape(groups, slabs, ch, 2, LANES).transpose(1, 2, 3, 0, 4)
        modes = modes.reshape(slabs, ch, 2, pens, owned).transpose(3, 0, 1, 2, 4)
        modes = modes.reshape(pens, slabs, ch, 2 * owned)
    modes = lax.all_to_all(modes, "pen", split_axis=0, concat_axis=0, tiled=True)
    modes = modes.reshape(nx, ch, 2 * owned)
    cos_x, sin_x = tables(nx, mx)
    forward_x = jnp.asarray((np.concatenate([cos_x, sin_x]) * nx**-0.5).astype(np.float32))
    waves = jnp.einsum("dx,xcl->dcl", forward_x, modes, precision=HIGHEST)
    real_x = waves[:mx, :, :owned] + waves[mx:, :, owned:]
    imag_x = waves[:mx, :, owned:] - waves[mx:, :, :owned]
    joined = lax.all_gather(
        jnp.concatenate([real_x, imag_x], axis=2), "ch", axis=1, tiled=True
    )
    real_x = joined[:, :, None, :owned]
    imag_x = joined[:, :, None, owned:]
    weight_re = spectral_weights[0, 0].astype(F32)
    weight_im = spectral_weights[0, 1].astype(F32)
    real_g = jnp.sum(real_x * weight_re - imag_x * weight_im, axis=1)
    imag_g = jnp.sum(imag_x * weight_re + real_x * weight_im, axis=1)
    mixed = lax.all_gather(jnp.concatenate([real_g, imag_g], axis=2), "pen", axis=0)
    if owned != LANES:
        mixed = mixed.reshape(pens, mx, ch, 2, owned).transpose(1, 2, 3, 0, 4)
        mixed = mixed.reshape(mx, ch, 2, groups, LANES).transpose(3, 0, 1, 2, 4)
        mixed = mixed.reshape(groups, mx, ch, 2 * LANES)
    inverse_x = jnp.asarray((np.concatenate([cos_x, sin_x]) * mx**-0.5).T.astype(np.float32))
    coefs = lax.dynamic_slice_in_dim(inverse_x, lax.axis_index("pen") * slabs, slabs, 0)
    first = (lax.axis_index("ch") * ch).astype(jnp.int32).reshape(1)
    return inverse_field(
        coefs, first, mixed, gathered, bypass_weights[0], bypass_bias, my, mz
    )


def solution(mesh):
    pens = mesh.shape["pen"]

    def run(features, spectral_weights, bypass_weights, bypass_bias):
        body = functools.partial(local, pens=pens, kept=spectral_weights.shape[5])
        return jax.shard_map(
            body,
            mesh=mesh,
            in_specs=(
                P(("grp", "pen"), "ch", None, None),
                P(None, None, None, None, "ch", "pen"),
                P(None, None, "ch"),
                P(None, "ch"),
            ),
            out_specs=P(("grp", "pen"), "ch", None, None),
            check_vma=False,
        )(features, spectral_weights, bypass_weights, bypass_bias)

    return run
```
